512 devices in a mesh: row: 16 (over z), col: 8 (over x, core), depth: 4 (over y).
Axes of the slice: x: 4, y: 4, z: 16, core: 2. Of those that a mesh axis runs over, the one named last changes fastest.
Arguments:
- eri_tiles: bfloat16 [192, 256, 128, 128], P('row', ('col', 'depth')), may hold values from -0.03125 to 0.03125
- screen: int32 [192, 256], P('row', ('col', 'depth')), may hold values from 0 to 1, as said below
- density_bra: bfloat16 [24576, 256], P('row', 'col'), may hold values from -6 to 6
- density_ket: bfloat16 [32768, 256], P(('col', 'depth'), 'row'), may hold values from -6 to 6
Outputs:
- coulomb_bra: float32 [24576, 256], P('row', 'col')
- coulomb_ket: float32 [32768, 256], P(('col', 'depth'), 'row')
The draws below stay inside these ranges and needn't reach their ends.
Inputs may be any that keep to these rules, and one draw needn't show every extreme that they name: `screen`: in each device's block of 12 x 8 tiles (aligned blocks), between 16 and 64 tiles are significant; some block has exactly 64.
All inputs are finite; a program needn't handle non-finite values.
Results may differ from the reference program's by a relative error of at most 0.005.
Values may be sent and summed in bfloat16 or wider, within the bound.
A program may use at most 64 MiB of HBM per device.

```python
import jax
import jax.numpy as jnp
from jax import lax

PAIR = 128
DENS = 256
A_DEV = 12
B_DEV = 8
NA = 192
NB = 256
CAP = 64


def draw_screen(key, part):
    blocks_r = NA // A_DEV
    blocks_c = NB // B_DEV
    tiles_dev = A_DEV * B_DEV
    devices_all = blocks_r * blocks_c
    lowest = max(1, CAP // 4)
    key_count, key_pick, key_perm = jax.random.split(jax.random.fold_in(key, 11), 3)
    counts = jax.random.randint(key_count, (devices_all,), lowest, CAP + 1)
    busiest = jax.random.randint(key_pick, (), 0, devices_all)
    counts = jnp.where(jnp.arange(devices_all) == busiest, CAP, counts)
    sub_keys = jax.random.split(key_perm, devices_all)

    def permute_one(subkey):
        return jax.random.permutation(subkey, tiles_dev)
    ranking = jax.vmap(permute_one)(sub_keys)
    significant = (ranking < counts[:, None]).astype(jnp.int32)
    return significant.reshape(blocks_r, blocks_c, A_DEV, B_DEV).transpose(0, 2, 1, 3).reshape(NA, NB)


def block_levels(rng, shape, shards, smallest, largest):
    def one(position, parts):
        steps = jax.random.uniform(jax.random.fold_in(jax.random.fold_in(rng, 6), position), (parts,), jnp.float32, smallest / len(shards), largest / len(shards))
        return jnp.repeat(jnp.exp(steps), shape[position] // parts).reshape((-1,) + (1,) * (len(shape) - position - 1))

    gain = one(*shards[0])
    for cut in shards[1:]:
        gain = gain * one(*cut)
    return gain


def noise(own_key, shape, scale, reach, cuts=(), kind=jnp.bfloat16):
    array = jax.random.normal(own_key, shape, jnp.float32) * scale
    if len(cuts) > 0:
        array = block_levels(own_key, shape, cuts, -0.22, 0.18) * array
    return jnp.clip(array, min=-reach, max=reach).astype(kind)


def setup_inputs(seed: int = 0) -> dict:
    arg_keys = jax.random.split(jax.random.key(seed), 5)
    return {
        "eri_tiles": noise(arg_keys[0], (NA, NB, PAIR, PAIR), (PAIR * (NA + NB) // 2) ** -0.5, 0.03125, ((0, 16), (1, 32))),
        "screen": draw_screen(jax.random.fold_in(arg_keys[4], 71), 0),
        "density_bra": noise(arg_keys[2], (NA * PAIR, DENS), 1.0, 6.0, ((0, 16), (1, 8))),
        "density_ket": noise(arg_keys[3], (NB * PAIR, DENS), 1.0, 6.0, ((0, 32), (1, 16))),
    }


def reference(eri_tiles, screen, density_bra, density_ket):
    keep = screen.astype(jnp.float32)
    ket_rows = density_ket.astype(jnp.float32).reshape(NB, PAIR, DENS)
    bra_rows = density_bra.astype(jnp.float32).reshape(NA, PAIR, DENS)

    def advance(carry, inputs):
        tiles, weights, bra_block = inputs
        masked = tiles.astype(jnp.float32) * weights[:, None, None]
        row_out = jnp.einsum('bij,bjr->ir', masked, ket_rows)
        carry = carry + jnp.einsum('bij,ir->bjr', masked, bra_block)
        return carry, row_out

    start_sum = jnp.zeros((NB, PAIR, DENS), jnp.float32)
    ket_total, bra_out = lax.scan(advance, start_sum, (eri_tiles, keep, bra_rows))
    return bra_out.reshape(NA * PAIR, DENS), ket_total.reshape(NB * PAIR, DENS)
```

```python
import jax
import jax.numpy as jnp
from jax import lax
from jax.experimental import pallas as pl
from jax.experimental.pallas import tpu as pltpu
from jax.sharding import PartitionSpec as P

MESH = pl.DeviceIdType.MESH
F32 = jnp.float32
BF16 = jnp.bfloat16

NZ, NX, NY = 16, 4, 4
NA_DEV, NB_DEV, PAIR = 12, 8, 128
ROWS_A, ROWS_B = NA_DEV * PAIR, NB_DEV * PAIR
HALF_A, HALF_B = ROWS_A // 2, ROWS_B // 2
STRIP = 16

PARENT = {}
for sign in (1, -1):
    for dist in (1, 2):
        PARENT[sign * dist] = 0
    for dist in range(3, 9):
        PARENT[sign * dist] = sign * (2 * ((dist - 1) // 2))
LEVELS = ((1, -1, 2, -2), (3, -3, 4, -4), (5, -5, 6, -6), (7, -7, 8, -8))
GROUPS = ((0, 1, -1, 2, -2), (3, -3, 4, -4), (5, -5, 6, -6), (7, -7, 8))


def kernel(
    eri_hbm, screen_ref, bra_hbm, ket_hbm,
    out_bra, out_ket,
    tiles, matrix, dbra, dket, ket_acc, rs_recv, rs_send,
    bra_part, bra_recv, bra_red, x_recv, y_sum, y_recv, f_sum, f_recv,
    load_sem, tile_sem,
    ag_send, ag_recv, x_send, x_rsem, d_send, d_recv,
    rs_ssem, rs_rsem, c_send, c_recv, xr_send, xr_recv, y_send, y_rsem, f_send, f_rsem,
):
    z = lax.axis_index("row")
    col = lax.axis_index("col")
    y = lax.axis_index("depth")
    x = col // 2
    core = lax.rem(col, 2)
    other = 1 - core

    def z_at(offset):
        return lax.rem(z + offset + 2 * NZ, NZ)

    def x_at(offset):
        return lax.rem(x + offset, NX)

    def y_at(offset):
        return lax.rem(y + offset, NY)

    def remote(src, dst, ssem, rsem, **where):
        return pltpu.make_async_remote_copy(
            src_ref=src, dst_ref=dst, send_sem=ssem, recv_sem=rsem,
            device_id=where, device_id_type=MESH,
        )

    loads = [pltpu.make_async_copy(bra_hbm, dbra.at[col], load_sem.at[0])]
    for h in range(2):
        loads.append(
            pltpu.make_async_copy(
                ket_hbm.at[:, pl.ds(h * HALF_B, HALF_B)], dket.at[z, h], load_sem.at[1 + h]
            )
        )
    for copy in loads:
        copy.start()
    tile_loads = [
        pltpu.make_async_copy(eri_hbm.at[a], tiles.at[a], tile_sem.at[a]) for a in range(NA_DEV)
    ]
    for copy in tile_loads:
        copy.start()

    barrier = pltpu.get_barrier_semaphore()
    peers = []
    for step in (1, -1, 2, -2):
        peers.append({"row": z_at(step)})
    for offset in range(1, NX):
        peers.append({"col": 2 * x_at(offset) + core})
    peers.append({"col": 2 * x + other})
    for offset in range(1, NY):
        peers.append({"depth": y_at(offset), "col": 2 * x})
        peers.append({"depth": y_at(offset), "col": 2 * x + 1})
    for peer in peers:
        pl.semaphore_signal(barrier, inc=1, device_id=peer, device_id_type=MESH)
    pl.semaphore_wait(barrier, len(peers))

    for copy in loads:
        copy.wait()

    sends = []
    for offset in (2, 1, 3):
        copy = remote(
            dbra.at[col], dbra.at[col], x_send.at[offset - 1], x_rsem.at[offset - 1],
            col=2 * x_at(offset) + core,
        )
        copy.start()
        sends.append(copy)
    copy = remote(dbra.at[col], dbra.at[col], d_send.at[0], d_recv.at[0], col=2 * x + other)
    copy.start()
    sends.append(copy)

    def ag_copy(offset):
        parent = PARENT[offset]
        slot = z_at(-parent)
        if abs(offset) == 8:
            h = 0 if offset > 0 else 1
            src, dst = dket.at[slot, h], dket.at[slot, h]
        else:
            src, dst = dket.at[slot], dket.at[slot]
        index = offset + 8
        return remote(src, dst, ag_send.at[index], ag_recv.at[index], row=z_at(offset - parent))

    def ag_wait(offset):
        slot = z_at(-offset)
        if abs(offset) == 8:
            ref = dket.at[slot, 0 if offset > 0 else 1]
        else:
            ref = dket.at[slot]
        index = offset + 8
        remote(ref, ref, ag_send.at[index], ag_recv.at[index], row=z_at(1)).wait_recv()

    def ag_forward(offset):
        for child, parent in PARENT.items():
            if parent == offset:
                copy = ag_copy(child)
                copy.start()
                sends.append(copy)

    ag_forward(0)

    for a in range(NA_DEV):
        tile_loads[a].wait()
        for b in range(NB_DEV):
            keep = screen_ref[b, a] > 0
            matrix[a * PAIR : (a + 1) * PAIR, b * PAIR : (b + 1) * PAIR] = jnp.where(
                keep, tiles[a, b], jnp.zeros((PAIR, PAIR), BF16)
            )

    def ket_group(xs):
        rows = jnp.concatenate([dbra[2 * xx + i] for xx in xs for i in range(2)], axis=0)
        for n in range(4):
            part = jnp.dot(
                rows, matrix[:, n * 256 : (n + 1) * 256], preferred_element_type=F32
            )
            for g, xx in enumerate(xs):
                for q in range(4):
                    lo = (4 * g + q) * STRIP
                    ket_acc[4 * xx + q, n // 2, :, (n % 2) * 256 : (n % 2 + 1) * 256] = part[
                        lo : lo + STRIP
                    ]

    def ag_level(level):
        for offset in LEVELS[level]:
            ag_wait(offset)
            ag_forward(offset)

    def d_copy(index, column):
        return remote(
            dbra.at[column], dbra.at[column], d_send.at[index], d_recv.at[index], col=2 * x + other
        )

    d_copy(0, 2 * x + other).wait_recv()
    ket_group([x])
    ag_level(0)
    for offset in (1, 3, 2):
        source = 2 * x_at(NX - offset)
        remote(
            dbra.at[source + core], dbra.at[source + core],
            x_send.at[offset - 1], x_rsem.at[offset - 1], col=2 * x + other,
        ).wait_recv()
        copy = d_copy(offset, source + core)
        copy.start()
        sends.append(copy)
    ag_level(1)
    for offset in (1, 3, 2):
        d_copy(offset, 2 * x_at(NX - offset) + other).wait_recv()
    ket_group([x_at(3), x_at(1), x_at(2)])

    def rs_copy(way, step, h, src):
        sign = 1 - 2 * way
        return remote(
            src, rs_recv.at[way, step - 1, h],
            rs_ssem.at[way, step - 1, h], rs_rsem.at[way, step - 1, h], row=z_at(sign),
        )

    def rs_exists(way, step, h):
        return step >= 2 or h == way

    def rs_step(step):
        for h in range(2):
            for way in range(2):
                if not rs_exists(way, step, h):
                    continue
                target = z_at((1 - 2 * way) * (9 - step))
                if step >= 2 and rs_exists(way, step - 1, h):
                    rs_copy(way, step - 1, h, rs_recv.at[way, step - 2, h]).wait_recv()
                    rs_send[way, step - 1, h] = ket_acc[target, h] + rs_recv[way, step - 2, h]
                    src = rs_send.at[way, step - 1, h]
                else:
                    src = ket_acc.at[target, h]
                copy = rs_copy(way, step, h, src)
                copy.start()
                sends.append(copy)

    def c_copy(offset, slot, h):
        return remote(
            bra_part.at[slot, h], bra_recv.at[slot],
            c_send.at[offset + 7], c_recv.at[offset + 7], col=2 * x + other,
        )

    def bra_group(group):
        slots = [z_at(-offset) for offset in group]
        rows = jnp.concatenate(
            [jnp.concatenate([dket[slot, 0], dket[slot, 1]], axis=1) for slot in slots], axis=0
        )
        for n in range(6):
            part = lax.dot_general(
                rows, matrix[n * 256 : (n + 1) * 256, :],
                (((1,), (1,)), ((), ())), preferred_element_type=F32,
            )
            for i, slot in enumerate(slots):
                bra_part[slot, n // 3, :, (n % 3) * 256 : (n % 3 + 1) * 256] = part[
                    i * STRIP : (i + 1) * STRIP
                ]
        for offset, slot in zip(group, slots):
            copy = c_copy(offset, slot, other)
            copy.start()
            sends.append(copy)

    def xr_copy(offset, slot):
        target = slot // 4
        away = lax.rem(target - x + NX, NX)
        index = lax.max(away - 1, 0)
        return away, remote(
            bra_red.at[slot], x_recv.at[index, lax.rem(slot, 4)],
            xr_send.at[offset + 7], xr_recv.at[index, lax.rem(slot, 4)],
            col=2 * target + core,
        )

    def bra_reduce(group):
        for offset in group:
            slot = z_at(-offset)
            c_copy(offset, slot, core).wait_recv()
            bra_red[slot] = bra_part[slot, core] + bra_recv[slot]
            away, copy = xr_copy(offset, slot)

            @pl.when(away != 0)
            def _():
                copy.start()

    rs_step(1)
    bra_group(GROUPS[0])
    ag_level(2)
    rs_step(2)
    bra_reduce(GROUPS[0])
    bra_group(GROUPS[1])
    rs_step(3)
    ag_level(3)
    bra_reduce(GROUPS[1])
    bra_group(GROUPS[2])
    rs_step(4)
    bra_reduce(GROUPS[2])
    bra_group(GROUPS[3])
    rs_step(5)
    bra_reduce(GROUPS[3])

    def y_copy(offset):
        target = y_at(offset)
        return remote(
            y_sum.at[target], y_recv.at[offset - 1], y_send.at[offset - 1], y_rsem.at[offset - 1],
            depth=target,
        )

    rs_step(6)
    for q in range(4):
        total = bra_red[4 * x + q]
        for index in range(3):
            remote(
                bra_red.at[4 * x + q], x_recv.at[index, q], xr_send.at[0], xr_recv.at[index, q],
                col=2 * x_at(1) + core,
            ).wait_recv()
            total = total + x_recv[index, q]
        y_sum[q] = total
    for offset in (2, 1, 3):
        copy = y_copy(offset)
        copy.start()
        sends.append(copy)
    rs_step(7)
    rs_step(8)
    total = y_sum[y]
    for offset in (1, 3, 2):
        y_copy(offset).wait_recv()
        total = total + y_recv[offset - 1]
    f_sum[...] = total
    owner = y // 2
    piece = 2 * lax.rem(y, 2) + core

    def f_copy(offset):
        return remote(
            f_sum, f_recv.at[piece], f_send.at[offset], f_rsem.at[piece],
            depth=y_at(offset), col=2 * x + owner,
        )

    for offset in (2, 1, 3):
        copy = f_copy(offset)
        copy.start()
        sends.append(copy)

    @pl.when(owner != core)
    def _():
        f_copy(0).start()

    @pl.when(owner == core)
    def _():
        f_recv[piece] = total

    for h in range(2):
        total = ket_acc[z, h]
        for way in range(2):
            rs_copy(way, 8, h, rs_recv.at[way, 7, h]).wait_recv()
            total = total + rs_recv[way, 7, h]
        out_ket[:, h * HALF_B : (h + 1) * HALF_B] = total

    for p in range(4):
        mine = jnp.logical_and(owner == core, piece == p)

        @pl.when(jnp.logical_not(mine))
        def _():
            remote(f_sum, f_recv.at[p], f_send.at[0], f_rsem.at[p], depth=y_at(1), col=col).wait_recv()

        out_bra[
            (p // 2) * STRIP : (p // 2 + 1) * STRIP, (p % 2) * HALF_A : (p % 2 + 1) * HALF_A
        ] = f_recv[p]

    for copy in sends:
        copy.wait_send()
    for group in GROUPS:
        for offset in group:
            away, copy = xr_copy(offset, z_at(-offset))

            @pl.when(away != 0)
            def _():
                copy.wait_send()

    @pl.when(owner != core)
    def _():
        f_copy(0).wait_send()


def body(eri_tiles, screen, density_bra, density_ket):
    any_spec = pl.BlockSpec(memory_space=pl.ANY)
    vmem_spec = pl.BlockSpec(memory_space=pltpu.VMEM)
    dma = pltpu.SemaphoreType.DMA
    bra_t, ket_t = pl.pallas_call(
        kernel,
        out_shape=(
            jax.ShapeDtypeStruct((32, ROWS_A), F32),
            jax.ShapeDtypeStruct((STRIP, ROWS_B), F32),
        ),
        in_specs=[any_spec, pl.BlockSpec(memory_space=pltpu.SMEM), any_spec, any_spec],
        out_specs=(vmem_spec, vmem_spec),
        scratch_shapes=[
            pltpu.VMEM((NA_DEV, NB_DEV, PAIR, PAIR), BF16),
            pltpu.VMEM((ROWS_A, ROWS_B), BF16),
            pltpu.VMEM((8, 32, ROWS_A), BF16),
            pltpu.VMEM((NZ, 2, STRIP, HALF_B), BF16),
            pltpu.VMEM((NZ, 2, STRIP, HALF_B), F32),
            pltpu.VMEM((2, 8, 2, STRIP, HALF_B), F32),
            pltpu.VMEM((2, 8, 2, STRIP, HALF_B), F32),
            pltpu.VMEM((NZ, 2, STRIP, HALF_A), F32),
            pltpu.VMEM((NZ, STRIP, HALF_A), F32),
            pltpu.VMEM((NZ, STRIP, HALF_A), F32),
            pltpu.VMEM((3, 4, STRIP, HALF_A), F32),
            pltpu.VMEM((4, STRIP, HALF_A), F32),
            pltpu.VMEM((3, STRIP, HALF_A), F32),
            pltpu.VMEM((STRIP, HALF_A), F32),
            pltpu.VMEM((4, STRIP, HALF_A), F32),
            dma((3,)),
            dma((NA_DEV,)),
            dma((17,)),
            dma((17,)),
            dma((3,)),
            dma((3,)),
            dma((4,)),
            dma((4,)),
            dma((2, 8, 2)),
            dma((2, 8, 2)),
            dma((16,)),
            dma((16,)),
            dma((16,)),
            dma((3, 4)),
            dma((3,)),
            dma((3,)),
            dma((4,)),
            dma((4,)),
        ],
        compiler_params=pltpu.CompilerParams(
            collective_id=0, has_side_effects=True, vmem_limit_bytes=67043328
        ),
    )(eri_tiles, screen.T, density_bra.T, density_ket.T)
    return bra_t.T, ket_t.T


def solution(mesh):
    return jax.shard_map(
        body,
        mesh=mesh,
        in_specs=(
            P("row", ("col", "depth"), None, None),
            P("row", ("col", "depth")),
            P("row", "col"),
            P(("col", "depth"), "row"),
        ),
        out_specs=(P("row", "col"), P(("col", "depth"), "row")),
        check_vma=False,
    )
```
